32 devices in a mesh: blk: 8 (over z, x), field: 4 (over y, core).
Axes of the slice: x: 2, y: 2, z: 4, core: 2. Of those that a mesh axis runs over, the one named last changes fastest.
Arguments:
- vectors: float32 [512, 32768], P('blk', 'field'), may hold values from 0 to 10
- section: int32 [1], replicated, may hold values from 0 to 7
Outputs:
- metrics: float32 [512, 4, 64], P('blk', None, 'field')
The draws below stay inside these ranges and needn't reach their ends.
All inputs are finite; a program needn't handle non-finite values.
Results may differ from the reference program's by a relative error of at most 0.0003.
Values sent between devices are 32-bit elements; how exact they have to be, the bound alone decides.
No kernel may reach another device: no remote copies, remote signals or barrier semaphores. Data moves between devices by JAX's collectives and lax.ppermute only.
A program may use at most 64 MiB of HBM per device.

```python
import math
import jax
import jax.numpy as jnp
from jax import lax

FIELDS = 32768
V_DEV = 64
STEPS = 4
VECTORS = 512
N_BLK = 8


def draw_vectors(key, part):
    folded = jax.random.fold_in(key, 17)
    key_rows, key_cols, key_cells, key_mix, key_pattern = jax.random.split(folded, 5)
    population = 8
    row_scale = jnp.exp(jax.random.uniform(key_rows, (VECTORS, 1), jnp.float32) * math.log(10.0))
    col_scale = jnp.exp(jax.random.uniform(key_cols, (1, FIELDS), jnp.float32) * math.log(10.0))
    patterns = jax.random.uniform(key_pattern, (population, FIELDS), jnp.float32)
    mixing = jax.random.uniform(key_mix, (VECTORS, population), jnp.float32) ** 4 + 0.01
    roughness = jax.random.uniform(key_cells, (VECTORS, FIELDS), jnp.float32, 0.25, 1.0)
    mixing = mixing / jnp.sum(mixing, axis=1, keepdims=True)
    blended = jnp.dot(mixing, patterns, precision=lax.Precision.HIGHEST)
    return (row_scale * col_scale * blended * roughness * 0.1).astype(jnp.float32)


def setup_inputs(seed: int = 0) -> dict:
    streams_of = jax.random.split(jax.random.key(seed), 3)
    return {
        "vectors": draw_vectors(jax.random.fold_in(streams_of[2], 71), 0),
        "section": jax.random.randint(streams_of[1], (1,), 0, N_BLK).astype(jnp.int32),
    }


def reference(vectors, section):
    sums = jnp.sum(vectors, axis=1)
    blocks = vectors.reshape(N_BLK, V_DEV, FIELDS)
    block_sums = sums.reshape(N_BLK, V_DEV)

    def one_block(index):
        own = blocks[index]
        own_sums = block_sums[index]

        def one_slot(slot):
            partner = (index + section[0] + slot) % N_BLK
            other = blocks[partner]
            other_sums = block_sums[partner]

            def one_row(row):
                return jnp.sum(jnp.minimum(row[None, :], other), axis=1)

            numer = lax.map(one_row, own)
            return 2.0 * numer / (own_sums[:, None] + other_sums[None, :])

        return lax.map(one_slot, jnp.arange(STEPS, dtype=jnp.int32))

    result = lax.map(one_block, jnp.arange(N_BLK, dtype=jnp.int32))
    return result.transpose(0, 2, 1, 3).reshape(N_BLK * V_DEV, STEPS, V_DEV)
```

```python
from functools import partial

import jax
import jax.numpy as jnp
from jax import lax
from jax.experimental import pallas as pl
from jax.experimental.pallas import tpu as pltpu
from jax.sharding import PartitionSpec as P

STEPS = 4
LANES = 128
PACK = 16
GROUP = 4


def tree_sum(values):
    values = list(values)
    while len(values) > 1:
        paired = [a + b for a, b in zip(values[::2], values[1::2])]
        if len(values) % 2:
            paired.append(values[-1])
        values = paired
    return values[0]


def pair_kernel(section, x_ref, out_ref, packed, *, blocks, v_dev, width):
    b = pl.program_id(0)
    vectors, fields = x_ref.shape
    chunks = fields // LANES

    @pl.when(b == 0)
    def _():
        def convert(r, _):
            rows = pl.ds(pl.multiple_of(r * PACK, PACK), PACK)
            packed[rows, :] = x_ref[rows, :].astype(jnp.bfloat16)
            return 0

        lax.fori_loop(0, vectors // PACK, convert, 0)

    first = section[0] % blocks
    lane = lax.broadcasted_iota(jnp.int32, (PACK, LANES), 1)
    tiles = v_dev // PACK
    per_field = width // PACK

    def folded_sums(block):
        rows = pl.ds(pl.multiple_of(block * v_dev, v_dev), v_dev)
        folded = tree_sum(x_ref[rows, c * LANES:(c + 1) * LANES] for c in range(chunks))
        return lax.dot_general(
            jnp.ones((8, LANES), jnp.float32), folded, (((1,), (1,)), ((), ())),
            precision=lax.Precision.HIGHEST, preferred_element_type=jnp.float32,
        )

    partners = [(b + first + s) % blocks for s in range(STEPS)]
    row = lax.broadcasted_iota(jnp.int32, (8, v_dev), 0)
    tail = folded_sums(b)
    for s in range(STEPS):
        tail = jnp.where(row == 1 + s, folded_sums(partners[s]), tail)
    halves = LANES // v_dev
    tail = jnp.concatenate([tail] * halves, axis=1)
    n_field = v_dev // width
    body = STEPS // halves * width
    for f in range(n_field):
        out_ref[0, f, body:body + 8, :] = tail

    for f in range(n_field):
        out_ref[0, f, 0:body, :] = jnp.zeros((body, LANES), jnp.float32)

    def over_rows(g, _):
        base = pl.multiple_of(b * v_dev + g * 8, 8)
        mine = [x_ref[pl.ds(base, 8), c * LANES:(c + 1) * LANES] for c in range(chunks)]
        for r0 in range(0, 8, GROUP):
            own = [
                [
                    jnp.broadcast_to(mine[c][r0 + r:r0 + r + 1], (PACK, LANES)).astype(jnp.bfloat16)
                    for c in range(chunks)
                ]
                for r in range(GROUP)
            ]
            for t in range(tiles):
                f, w = divmod(t, per_field)
                for s1 in range(STEPS // halves):
                    at = s1 * width + w * PACK
                    acc = out_ref[0, f, at:at + PACK, :]
                    for s0 in range(halves):
                        start = pl.multiple_of(partners[s1 * halves + s0] * v_dev + t * PACK, PACK)
                        other = [
                            packed[pl.ds(start, PACK), c * LANES:(c + 1) * LANES]
                            for c in range(chunks)
                        ]
                        for r in range(GROUP):
                            total = tree_sum(
                                jnp.minimum(own[r][c], other[c]) for c in range(chunks)
                            )
                            total = jnp.sum(total.astype(jnp.float32), axis=1, keepdims=True)
                            column = s0 * v_dev + g * 8 + r0 + r
                            acc = jnp.where(lane == column, total, acc)
                    out_ref[0, f, at:at + PACK, :] = acc
        return 0

    lax.fori_loop(0, v_dev // 8, over_rows, 0)


def pair_sums(x, section, blocks, n_field):
    vectors, fields = x.shape
    v_dev = vectors // blocks
    width = v_dev // n_field
    rows = STEPS * v_dev // LANES * width + 8
    return pl.pallas_call(
        partial(pair_kernel, blocks=blocks, v_dev=v_dev, width=width),
        out_shape=jax.ShapeDtypeStruct((blocks, n_field, rows, LANES), jnp.float32),
        grid_spec=pltpu.PrefetchScalarGridSpec(
            num_scalar_prefetch=1,
            grid=(blocks,),
            in_specs=[pl.BlockSpec((vectors, fields), lambda b, _: (0, 0))],
            out_specs=pl.BlockSpec((1, n_field, rows, LANES), lambda b, _: (b, 0, 0, 0)),
            scratch_shapes=[
                pltpu.VMEM((vectors, fields), jnp.bfloat16),
            ],
        ),
        compiler_params=pltpu.CompilerParams(
            dimension_semantics=("arbitrary",), vmem_limit_bytes=48 * 1024 * 1024
        ),
        name="pair_sums",
    )(section, x)


def per_device(vectors, section):
    blocks = lax.axis_size("blk")
    n_field = lax.axis_size("field")
    v_dev = vectors.shape[0]
    width = v_dev // n_field
    halves = LANES // v_dev
    x = lax.all_to_all(vectors, "blk", 1, 0, tiled=True)
    partial_sums = pair_sums(x, section, blocks, n_field)
    rows = partial_sums.shape[2]
    received = lax.all_to_all(
        partial_sums.reshape(blocks * n_field, rows, LANES), ("blk", "field"), 0, 0, tiled=True
    )
    whole = jnp.sum(received, axis=0)
    body = rows - 8
    numer = whole[:body].reshape(STEPS // halves, width, halves, v_dev)
    numer = numer.transpose(3, 0, 2, 1).reshape(v_dev, STEPS, width)
    own = whole[body, :v_dev]
    other = whole[body + 1:body + 1 + STEPS, :v_dev]
    other = lax.dynamic_slice_in_dim(other, lax.axis_index("field") * width, width, 1)
    return 2.0 * numer / (own[:, None, None] + other[None])


def solution(mesh):
    placed = (P("blk", "field"), P())
    return jax.shard_map(
        per_device, mesh=mesh, in_specs=placed, out_specs=P("blk", None, "field"), check_vma=False
    )
```

```python
from functools import partial

import jax
import jax.numpy as jnp
from jax import lax
from jax.experimental import pallas as pl
from jax.experimental.pallas import tpu as pltpu
from jax.sharding import PartitionSpec as P

STEPS = 4
LANES = 128
PACK = 16
GROUP = 8
PARTS = 1


def tree_sum(values):
    values = list(values)
    while len(values) > 1:
        paired = [a + b for a, b in zip(values[::2], values[1::2])]
        if len(values) % 2:
            paired.append(values[-1])
        values = paired
    return values[0]


def pair_kernel(place, *refs, blocks, v_dev, width, added):
    pieces, refs = refs[:blocks], refs[blocks:]
    earlier = refs[0] if added else None
    out_ref, x_ref, packed = refs[-3:]
    b = pl.program_id(0)
    fields = x_ref.shape[1]
    chunks = fields // LANES

    @pl.when(b == 0)
    def _():
        for d in range(blocks):
            source = (place[1] + blocks - d) % blocks
            rows = pl.ds(pl.multiple_of(source * v_dev, v_dev), v_dev)
            values = pieces[d][...]
            x_ref[rows, :] = values
            packed[rows, :] = values.astype(jnp.bfloat16)

    first = place[0]
    lane = lax.broadcasted_iota(jnp.int32, (PACK, LANES), 1)
    tiles = v_dev // PACK
    per_field = width // PACK

    def folded_sums(block):
        rows = pl.ds(pl.multiple_of(block * v_dev, v_dev), v_dev)
        folded = tree_sum(x_ref[rows, c * LANES:(c + 1) * LANES] for c in range(chunks))
        return lax.dot_general(
            jnp.ones((8, LANES), jnp.float32), folded, (((1,), (1,)), ((), ())),
            precision=lax.Precision.HIGHEST, preferred_element_type=jnp.float32,
        )

    partners = [(b + first + s) % blocks for s in range(STEPS)]
    row = lax.broadcasted_iota(jnp.int32, (8, v_dev), 0)
    tail = folded_sums(b)
    for s in range(STEPS):
        tail = jnp.where(row == 1 + s, folded_sums(partners[s]), tail)
    halves = LANES // v_dev
    tail = jnp.concatenate([tail] * halves, axis=1)
    n_field = v_dev // width
    body = STEPS // halves * width
    for f in range(n_field):
        out_ref[0, f, body:body + 8, :] = tail

    for f in range(n_field):
        out_ref[0, f, 0:body, :] = jnp.zeros((body, LANES), jnp.float32)

    def over_rows(g, _):
        base = pl.multiple_of(b * v_dev + g * 8, 8)
        mine = [x_ref[pl.ds(base, 8), c * LANES:(c + 1) * LANES] for c in range(chunks)]
        for r0 in range(0, 8, GROUP):
            own = [
                [
                    jnp.broadcast_to(mine[c][r0 + r:r0 + r + 1], (PACK, LANES)).astype(jnp.bfloat16)
                    for c in range(chunks)
                ]
                for r in range(GROUP)
            ]
            for t in range(tiles):
                f, w = divmod(t, per_field)
                for s1 in range(STEPS // halves):
                    at = s1 * width + w * PACK
                    acc = out_ref[0, f, at:at + PACK, :]
                    for s0 in range(halves):
                        start = pl.multiple_of(partners[s1 * halves + s0] * v_dev + t * PACK, PACK)
                        other = [
                            packed[pl.ds(start, PACK), c * LANES:(c + 1) * LANES]
                            for c in range(chunks)
                        ]
                        for r in range(GROUP):
                            total = tree_sum(
                                jnp.minimum(own[r][c], other[c]) for c in range(chunks)
                            )
                            total = jnp.sum(total.astype(jnp.float32), axis=1, keepdims=True)
                            column = s0 * v_dev + g * 8 + r0 + r
                            acc = jnp.where(lane == column, total, acc)
                    out_ref[0, f, at:at + PACK, :] = acc
        return 0

    lax.fori_loop(0, v_dev // 8, over_rows, 0)

    if added:
        out_ref[...] += earlier[...]


def pair_sums(pieces, place, blocks, n_field, earlier=None):
    v_dev, fields = pieces[0].shape
    vectors = v_dev * blocks
    width = v_dev // n_field
    rows = STEPS * v_dev // LANES * width + 8
    per_block = pl.BlockSpec((1, n_field, rows, LANES), lambda b, _: (b, 0, 0, 0))
    more = [] if earlier is None else [earlier]
    return pl.pallas_call(
        partial(pair_kernel, blocks=blocks, v_dev=v_dev, width=width, added=bool(more)),
        out_shape=jax.ShapeDtypeStruct((blocks, n_field, rows, LANES), jnp.float32),
        grid_spec=pltpu.PrefetchScalarGridSpec(
            num_scalar_prefetch=1,
            grid=(blocks,),
            in_specs=[pl.BlockSpec((v_dev, fields), lambda b, _: (0, 0))] * blocks
            + [per_block] * len(more),
            out_specs=per_block,
            scratch_shapes=[
                pltpu.VMEM((vectors, fields), jnp.float32),
                pltpu.VMEM((vectors, fields), jnp.bfloat16),
            ],
        ),
        compiler_params=pltpu.CompilerParams(
            dimension_semantics=("arbitrary",), vmem_limit_bytes=48 * 1024 * 1024
        ),
        name="pair_sums",
    )(place, *pieces, *more)


def per_device(vectors, section):
    blocks = lax.axis_size("blk")
    n_field = lax.axis_size("field")
    v_dev, fields = vectors.shape
    width = v_dev // n_field
    halves = LANES // v_dev
    share = fields // blocks
    parts = PARTS if share % (PARTS * LANES) == 0 else 1
    size = share // parts
    me = lax.axis_index("blk")
    place = jnp.stack([section[0] % blocks, me]).astype(jnp.int32)
    arrived = []
    for p in range(parts):
        pieces = []
        for d in range(blocks):
            to = (me + d) % blocks
            piece = lax.dynamic_slice_in_dim(vectors, to * share + p * size, size, 1)
            if d:
                piece = lax.ppermute(piece, "blk", [(s, (s + d) % blocks) for s in range(blocks)])
            pieces.append(piece)
        arrived.append(pieces)
    partial_sums = None
    for pieces in arrived:
        partial_sums = pair_sums(pieces, place, blocks, n_field, partial_sums)
    rows = partial_sums.shape[2]
    received = lax.all_to_all(
        partial_sums.reshape(blocks * n_field, rows, LANES), ("blk", "field"), 0, 0, tiled=True
    )
    whole = jnp.sum(received, axis=0)
    body = rows - 8
    numer = whole[:body].reshape(STEPS // halves, width, halves, v_dev)
    numer = numer.transpose(3, 0, 2, 1).reshape(v_dev, STEPS, width)
    own = whole[body, :v_dev]
    other = whole[body + 1:body + 1 + STEPS, :v_dev]
    other = lax.dynamic_slice_in_dim(other, lax.axis_index("field") * width, width, 1)
    return 2.0 * numer / (own[:, None, None] + other[None])


def solution(mesh):
    placed = (P("blk", "field"), P())
    return jax.shard_map(
        per_device, mesh=mesh, in_specs=placed, out_specs=P("blk", None, "field"), check_vma=False
    )
```

```python
from functools import partial

import jax
import jax.numpy as jnp
from jax import lax
from jax.experimental import pallas as pl
from jax.experimental.pallas import tpu as pltpu
from jax.sharding import PartitionSpec as P

STEPS = 4
LANES = 128
PACK = 16
GROUP = 8
PARTS = 1


def tree_sum(values):
    values = list(values)
    while len(values) > 1:
        paired = [a + b for a, b in zip(values[::2], values[1::2])]
        if len(values) % 2:
            paired.append(values[-1])
        values = paired
    return values[0]


def pair_kernel(place, *refs, blocks, v_dev, width, added):
    pieces, refs = refs[:blocks], refs[blocks:]
    earlier = refs[0] if added else None
    out_ref, x_ref, packed = refs[-3:]
    b = pl.program_id(0)
    fields = x_ref.shape[1]
    chunks = fields // LANES

    @pl.when(b == 0)
    def _():
        for d in range(blocks):
            source = (place[1] + blocks - d) % blocks
            rows = pl.ds(pl.multiple_of(source * v_dev, v_dev), v_dev)
            values = pieces[d][...]
            x_ref[rows, :] = values
            packed[rows, :] = values.astype(jnp.bfloat16)

    first = place[0]
    lane = lax.broadcasted_iota(jnp.int32, (PACK, LANES), 1)
    tiles = v_dev // PACK
    per_field = width // PACK

    def folded_sums(block):
        rows = pl.ds(pl.multiple_of(block * v_dev, v_dev), v_dev)
        folded = tree_sum(x_ref[rows, c * LANES:(c + 1) * LANES] for c in range(chunks))
        return lax.dot_general(
            jnp.ones((8, LANES), jnp.float32), folded, (((1,), (1,)), ((), ())),
            precision=lax.Precision.HIGHEST, preferred_element_type=jnp.float32,
        )

    partners = [(b + first + s) % blocks for s in range(STEPS)]
    row = lax.broadcasted_iota(jnp.int32, (8, v_dev), 0)
    tail = folded_sums(b)
    for s in range(STEPS):
        tail = jnp.where(row == 1 + s, folded_sums(partners[s]), tail)
    halves = LANES // v_dev
    tail = jnp.concatenate([tail] * halves, axis=1)
    n_field = v_dev // width
    body = STEPS // halves * width
    for f in range(n_field):
        out_ref[0, f, body:body + 8, :] = tail

    for f in range(n_field):
        out_ref[0, f, 0:body, :] = jnp.zeros((body, LANES), jnp.float32)

    def over_rows(g, _):
        base = pl.multiple_of(b * v_dev + g * 8, 8)
        mine = [x_ref[pl.ds(base, 8), c * LANES:(c + 1) * LANES] for c in range(chunks)]
        for r0 in range(0, 8, GROUP):
            own = [
                [
                    jnp.broadcast_to(mine[c][r0 + r:r0 + r + 1], (PACK, LANES)).astype(jnp.bfloat16)
                    for c in range(chunks)
                ]
                for r in range(GROUP)
            ]
            for t in range(tiles):
                f, w = divmod(t, per_field)
                for s1 in range(STEPS // halves):
                    at = s1 * width + w * PACK
                    acc = out_ref[0, f, at:at + PACK, :]
                    for s0 in range(halves):
                        start = pl.multiple_of(partners[s1 * halves + s0] * v_dev + t * PACK, PACK)
                        other = [
                            packed[pl.ds(start, PACK), c * LANES:(c + 1) * LANES]
                            for c in range(chunks)
                        ]
                        for r in range(GROUP):
                            total = tree_sum(
                                jnp.minimum(own[r][c], other[c]) for c in range(chunks)
                            )
                            total = jnp.sum(total.astype(jnp.float32), axis=1, keepdims=True)
                            column = s0 * v_dev + g * 8 + r0 + r
                            acc = jnp.where(lane == column, total, acc)
                    out_ref[0, f, at:at + PACK, :] = acc
        return 0

    lax.fori_loop(0, v_dev // 8, over_rows, 0)

    if added:
        out_ref[...] += earlier[...]


def pair_sums(pieces, place, blocks, n_field, earlier=None):
    v_dev, fields = pieces[0].shape
    vectors = v_dev * blocks
    width = v_dev // n_field
    rows = STEPS * v_dev // LANES * width + 8
    per_block = pl.BlockSpec((1, n_field, rows, LANES), lambda b, _: (b, 0, 0, 0))
    more = [] if earlier is None else [earlier]
    return pl.pallas_call(
        partial(pair_kernel, blocks=blocks, v_dev=v_dev, width=width, added=bool(more)),
        out_shape=jax.ShapeDtypeStruct((blocks, n_field, rows, LANES), jnp.float32),
        grid_spec=pltpu.PrefetchScalarGridSpec(
            num_scalar_prefetch=1,
            grid=(blocks,),
            in_specs=[pl.BlockSpec((v_dev, fields), lambda b, _: (0, 0))] * blocks
            + [per_block] * len(more),
            out_specs=per_block,
            scratch_shapes=[
                pltpu.VMEM((vectors, fields), jnp.float32),
                pltpu.VMEM((vectors, fields), jnp.bfloat16),
            ],
        ),
        compiler_params=pltpu.CompilerParams(
            dimension_semantics=("arbitrary",), vmem_limit_bytes=48 * 1024 * 1024
        ),
        name="pair_sums",
    )(place, *pieces, *more)


def per_device(vectors, section):
    blocks = lax.axis_size("blk")
    n_field = lax.axis_size("field")
    v_dev, fields = vectors.shape
    width = v_dev // n_field
    halves = LANES // v_dev
    share = fields // blocks
    parts = PARTS if share % (PARTS * LANES) == 0 else 1
    size = share // parts
    me = lax.axis_index("blk")
    place = jnp.stack([section[0] % blocks, me]).astype(jnp.int32)
    arrived = []
    for p in range(parts):
        pieces = []
        for d in range(blocks):
            to = (me + d) % blocks
            piece = lax.dynamic_slice_in_dim(vectors, to * share + p * size, size, 1)
            hops = [-(blocks // 4), d - 3 * blocks // 4] if d in (blocks // 2, blocks // 2 + 1) and blocks % 4 == 0 else [d]
            for hop in hops if d else []:
                piece = lax.ppermute(piece, "blk", [(s, (s + hop) % blocks) for s in range(blocks)])
            pieces.append(piece)
        arrived.append(pieces)
    partial_sums = None
    for pieces in arrived:
        partial_sums = pair_sums(pieces, place, blocks, n_field, partial_sums)
    rows = partial_sums.shape[2]
    received = lax.all_to_all(
        partial_sums.reshape(blocks * n_field, rows, LANES), ("blk", "field"), 0, 0, tiled=True
    )
    whole = jnp.sum(received, axis=0)
    body = rows - 8
    numer = whole[:body].reshape(STEPS // halves, width, halves, v_dev)
    numer = numer.transpose(3, 0, 2, 1).reshape(v_dev, STEPS, width)
    own = whole[body, :v_dev]
    other = whole[body + 1:body + 1 + STEPS, :v_dev]
    other = lax.dynamic_slice_in_dim(other, lax.axis_index("field") * width, width, 1)
    return 2.0 * numer / (own[:, None, None] + other[None])


def solution(mesh):
    placed = (P("blk", "field"), P())
    return jax.shard_map(
        per_device, mesh=mesh, in_specs=placed, out_specs=P("blk", None, "field"), check_vma=False
    )
```
